256 devices in a mesh: sec: 16 (over z_hi, x, core), gy: 4 (over z_lo), gz: 4 (over y).
Axes of the slice: x: 4, y: 4, z: 8 (z_hi: 2, z_lo: 4; z = z_hi * 4 + z_lo), core: 2. Of those that a mesh axis runs over, the one named last changes fastest.
Arguments:
- inflow: float32 [5, 128, 1024], P(None, 'gy', 'gz'), may hold values from -6 to 6
- initial: float32 [16, 5, 128, 1024], P('sec', None, 'gy', 'gz'), may hold values from -6 to 6
- solid: int32 [16, 128, 1024], P('sec', 'gy', 'gz'), may hold values 0 or 1
- speed_y: float32 [5], replicated, may hold values from -1 to 1
- speed_z: float32 [5], replicated, may hold values from -1 to 1
- vigneron: float32 [5], replicated, may hold values from 0.2 to 0.9
- coupling: float32 [5, 5], replicated, may hold values from -2.5 to 2.5
Outputs:
- marched: float32 [16, 5, 128, 1024], P('sec', None, 'gy', 'gz')
The draws below stay inside these ranges and needn't reach their ends.
Inputs may be any that keep to these rules, and one draw needn't show every extreme that they name: `solid`: 1 marks a cell inside the body, 0 a fluid cell.
All inputs are finite; a program needn't handle non-finite values. No bound on the sum of `solid` on one device may be relied on, other than what follows from the above.
Results may differ from the reference program's by a relative error of at most 0.00025.
Values sent between devices are 32-bit elements; how exact they have to be, the bound alone decides.
A program may use at most 64 MiB of HBM per device.

```python
import jax
import jax.numpy as jnp
from jax import lax

NVAR = 5
ITERS = 4
CORRECTORS = 3
NEWTON = 2
NSEC = 16
NY = 128
NZ = 1024


def place_ends(values, key, low, top_value):
    longest = values.shape.index(max(values.shape))
    spots = []
    for shift in (0, 1):
        where = [jax.random.randint(jax.random.fold_in(key, axis), (), 0, length) for axis, length in enumerate(values.shape)]
        where[longest] = (where[longest] + shift) % values.shape[longest]
        spots.append(tuple(where))
    return values.at[spots[0]].set(low).at[spots[1]].set(top_value)


def steps_of(key, shape, pieces, least, largest):
    loudness, own = 1.0, jax.random.fold_in(key, 6)
    for position, shards_of in pieces:
        draws = jnp.exp(jax.random.uniform(jax.random.fold_in(own, position), (shards_of,), jnp.float32, least / len(pieces), largest / len(pieces)))
        loudness = loudness * jnp.repeat(draws, shape[position] // shards_of).reshape([-1 if axis == position else 1 for axis in range(len(shape))])
    return loudness


def gaussian(rng, dims, scale, reach, cuts=(), held_as=jnp.bfloat16):
    entries = jax.random.normal(rng, dims, jnp.float32) * scale
    if len(cuts) > 0:
        entries = steps_of(rng, dims, cuts, -0.22, 0.18) * entries
    return jnp.clip(entries, min=-reach, max=reach).astype(held_as)


def setup_inputs(seed: int = 0) -> dict:
    streams_of = jax.random.split(jax.random.key(seed), 8)
    return {
        "inflow": gaussian(streams_of[0], (NVAR, NY, NZ), 1.0, 6.0, ((1, 4), (2, 4)), jnp.float32),
        "initial": gaussian(streams_of[1], (NSEC, NVAR, NY, NZ), 1.0, 6.0, ((0, 16), (2, 4), (3, 4)), jnp.float32),
        "solid": place_ends((jax.random.randint(streams_of[2], (NSEC, NY, NZ), 0, 8) < 1).astype(jnp.int32), jax.random.fold_in(streams_of[2], 1), 0, 1),
        "speed_y": jnp.clip(jax.random.uniform(streams_of[3], (NVAR,), jnp.float32, -1.0, 1.0), -1.0, 1.0),
        "speed_z": jnp.clip(jax.random.uniform(streams_of[4], (NVAR,), jnp.float32, -1.0, 1.0), -1.0, 1.0),
        "vigneron": jnp.clip(jax.random.uniform(streams_of[5], (NVAR,), jnp.float32, 0.2, 0.9), 0.2, 0.9),
        "coupling": gaussian(streams_of[6], (NVAR, NVAR), NVAR ** -0.5, 2.5, (), jnp.float32),
    }


STEP_RATIO = 0.25
WENO_EPS = 1e-6


def weno_face(left_far, left_near, center, right_near, right_far):
    smooth_left = (13.0 / 12.0) * (left_far - 2.0 * left_near + center) ** 2 + 0.25 * (left_far - 4.0 * left_near + 3.0 * center) ** 2
    smooth_middle = (13.0 / 12.0) * (left_near - 2.0 * center + right_near) ** 2 + 0.25 * (left_near - right_near) ** 2
    smooth_right = (13.0 / 12.0) * (center - 2.0 * right_near + right_far) ** 2 + 0.25 * (3.0 * center - 4.0 * right_near + right_far) ** 2
    weight_left = 0.1 / (WENO_EPS + smooth_left) ** 2
    weight_middle = 0.6 / (WENO_EPS + smooth_middle) ** 2
    weight_right = 0.3 / (WENO_EPS + smooth_right) ** 2
    guess_left = (2.0 * left_far - 7.0 * left_near + 11.0 * center) / 6.0
    guess_middle = (-left_near + 5.0 * center + 2.0 * right_near) / 6.0
    guess_right = (2.0 * center + 5.0 * right_near - right_far) / 6.0
    total = weight_left * guess_left + weight_middle * guess_middle + weight_right * guess_right
    return total / (weight_left + weight_middle + weight_right)


def sweep(padded, speeds, axis):
    count = padded.shape[axis] - 6
    plus_flux = jnp.maximum(speeds, 0.0)[:, None, None] * padded
    minus_flux = jnp.minimum(speeds, 0.0)[:, None, None] * padded

    def window(source, offset):
        return lax.slice_in_dim(source, offset, offset + count + 1, axis=axis)

    faces = weno_face(window(plus_flux, 0), window(plus_flux, 1), window(plus_flux, 2), window(plus_flux, 3), window(plus_flux, 4))
    faces = faces + weno_face(window(minus_flux, 5), window(minus_flux, 4), window(minus_flux, 3), window(minus_flux, 2), window(minus_flux, 1))
    return lax.slice_in_dim(faces, 1, count + 1, axis=axis) - lax.slice_in_dim(faces, 0, count, axis=axis)


def crossflow(padded, speed_y, speed_z):
    rows_part = sweep(padded[:, :, 3:-3], speed_y, 1)
    cols_part = sweep(padded[:, 3:-3, :], speed_z, 2)
    return rows_part + cols_part


def streamwise(field, factor):
    return field + factor * field ** 3 / (1.0 + field ** 2)


def slope(field, factor):
    return 1.0 + factor * field ** 2 * (3.0 + field ** 2) / (1.0 + field ** 2) ** 2


def correct(padded, current, upstream, diff, blocked, params):
    speed_y, speed_z, vigneron, coupling = params
    factor = vigneron[:, None, None]
    mixed = jnp.einsum("vw,wyz->vyz", coupling, current, precision=lax.Precision.HIGHEST)
    target = streamwise(upstream, factor) - STEP_RATIO * crossflow(padded, speed_y, speed_z) + STEP_RATIO * mixed - (1.0 - factor) * diff
    guess = current
    for newton_index in range(NEWTON):
        guess = guess - (streamwise(guess, factor) - target) / slope(guess, factor)
    return jnp.where(blocked[None], 0.0, guess)


def station(upstream, diff, blocked, params):
    current = upstream
    for corrector_index in range(CORRECTORS):
        padded = jnp.pad(current, ((0, 0), (3, 3), (3, 3)))
        current = correct(padded, current, upstream, diff, blocked, params)
    return current


def reference(inflow, initial, solid, speed_y, speed_z, vigneron, coupling):
    params = (speed_y, speed_z, vigneron, coupling)
    solid_cells = solid != 0
    planes = initial
    for iterate in range(ITERS):
        prior_upstream = jnp.concatenate([inflow[None], planes[:-1]], axis=0)

        def march(upstream, inputs):
            prior_here, prior_above, solid_here = inputs
            updated = station(upstream, prior_here - prior_above, solid_here, params)
            return updated, updated

        final_plane, planes = lax.scan(march, inflow, (planes, prior_upstream, solid_cells))
    return planes
```

```python
import jax
import jax.numpy as jnp
from jax import lax
from jax.experimental import pallas as pl
from jax.experimental.pallas import tpu as pltpu
from jax.sharding import PartitionSpec as P

ITERS = 4
CORRECTORS = 3
NEWTON = 2
NVAR = 5
STEP_RATIO = 0.25
WENO_EPS = 1e-06
ROWS = 32
LANES = 128
TOP = 8
MESH = pl.DeviceIdType.MESH


def inverse(x):
    r = pl.reciprocal(x, approx=True)
    return r * (2.0 - x * r)


def direction(speed):
    pos = speed >= 0.0

    def pick(a, b):
        return jnp.where(pos, jnp.float32(a), jnp.float32(b))

    return dict(
        s2=speed * speed,
        left=pick(1 / 6, 0.5),
        right=pick(0.5, 1 / 6),
        l1=pick(5 / 6, -4 / 6),
        l2=pick(-2 / 6, 1 / 6),
        m1=pick(1 / 6, -2 / 6),
        m2=pick(2 / 6, -1 / 6),
        r1=pick(4 / 6, -5 / 6),
        r2=pick(-1 / 6, 2 / 6),
    )


def face(a, b, c, d, e, k):
    ba, cb, dc, ed = b - a, c - b, d - c, e - d
    s2 = k["s2"]

    def weight(second, first):
        smooth = (13.0 / 3.0) * (second * second) + first * first
        r = inverse(4.0 * WENO_EPS + s2 * smooth)
        return r * r

    left2, mid2, right2 = cb - ba, dc - cb, ed - dc
    gl = k["left"] * weight(left2, left2 + 2.0 * cb)
    gm = weight(mid2, dc + cb)
    gr = k["right"] * weight(right2, right2 - 2.0 * dc)
    ql = k["l1"] * cb + k["l2"] * ba
    qm = k["m1"] * cb + k["m2"] * dc
    qr = k["r1"] * dc + k["r2"] * ed
    return c + (gl * ql + gm * qm + gr * qr) * inverse(gl + gm + gr)


def kernel(inflow, initial, solid, sy, sz, vig, coup, out,
           X, GA, BD, T0, ZS, ZR, ys_send, ys_recv, zs_send, zs_recv,
           pl_send, pl_recv, ga_send, ga_recv):
    p, y, z = lax.axis_index("sec"), lax.axis_index("gy"), lax.axis_index("gz")
    np_, ny, nz = lax.axis_size("sec"), lax.axis_size("gy"), lax.axis_size("gz")
    first, not_last = p == 0, p < np_ - 1
    sides = (
        ("y", 0, y > 0, y - 1, z), ("y", 1, y < ny - 1, y + 1, z),
        ("z", 0, z > 0, y, z - 1), ("z", 1, z < nz - 1, y, z + 1),
    )
    lane = lax.broadcasted_iota(jnp.int32, (8, LANES), 1)

    barrier = pltpu.get_barrier_semaphore()
    count = jnp.int32(0)
    for _, _, there, yy, zz in sides:
        count = count + there.astype(jnp.int32)

        @pl.when(there)
        def _():
            pl.semaphore_signal(barrier, inc=1, device_id=(p, yy, zz), device_id_type=MESH)

        @pl.when(there & (p > 0))
        def _():
            pl.semaphore_signal(barrier, inc=1, device_id=(p - 1, yy, zz), device_id_type=MESH)

    @pl.when(p > 0)
    def _():
        pl.semaphore_signal(barrier, inc=1, device_id=(p - 1, y, z), device_id_type=MESH)

    for kind, side, there, _, _ in sides:
        @pl.when(jnp.logical_not(there))
        def _():
            if kind == "y":
                at = 0 if side == 0 else TOP + ROWS
                zero = jnp.zeros((NVAR, 2, 8, LANES), jnp.float32)
                for k in range(ITERS):
                    for c in range(CORRECTORS):
                        X[k, c, :, :, at:at + 8, :] = zero
            else:
                for k in range(ITERS):
                    for c in range(CORRECTORS):
                        ZR[k, c, side] = jnp.zeros((8, LANES), jnp.float32)

    @pl.when(first)
    def _():
        for v in range(NVAR):
            for b in range(2):
                q = inflow[v, :, b * LANES:(b + 1) * LANES]
                for k in range(ITERS):
                    X[k, 0, v, b, TOP:TOP + ROWS, :] = q

    pl.semaphore_wait(barrier, count + not_last.astype(jnp.int32) * (1 + count))

    def ga_copy():
        return pltpu.make_async_remote_copy(
            src_ref=initial.at[0], dst_ref=GA, send_sem=ga_send, recv_sem=ga_recv,
            device_id=(p + 1, y, z), device_id_type=MESH)

    def plane_copy(k, v):
        return pltpu.make_async_remote_copy(
            src_ref=X.at[k, 3, v, :, TOP:TOP + ROWS, :],
            dst_ref=X.at[k, 0, v, :, TOP:TOP + ROWS, :],
            send_sem=pl_send.at[k, v], recv_sem=pl_recv.at[k, v],
            device_id=(p + 1, y, z), device_id_type=MESH)

    def side_copy(kind, side, k, source, slot, target):
        other = 1 - side
        if kind == "y":
            src = TOP if side == 0 else TOP + ROWS - 8
            dst = TOP + ROWS if side == 0 else 0
            return pltpu.make_async_remote_copy(
                src_ref=X.at[k, source, :, :, src:src + 8, :],
                dst_ref=X.at[k, slot, :, :, dst:dst + 8, :],
                send_sem=ys_send.at[k, source, side], recv_sem=ys_recv.at[k, slot, other],
                device_id=target, device_id_type=MESH)
        return pltpu.make_async_remote_copy(
            src_ref=ZS.at[k, source, side], dst_ref=ZR.at[k, slot, other],
            send_sem=zs_send.at[k, source, side], recv_sem=zs_recv.at[k, slot, other],
            device_id=target, device_id_type=MESH)

    def pack(k, source):
        low = jnp.zeros((8, LANES), jnp.float32)
        high = jnp.zeros((8, LANES), jnp.float32)
        for i in range(NVAR * 4):
            v, g = divmod(i, 4)
            rows = slice(TOP + 8 * g, TOP + 8 * g + 8)
            mine = (lane >= 4 * i) & (lane < 4 * i + 4)
            a = X[k, source, v, 0, rows, :]
            b = X[k, source, v, 1, rows, :]
            low = jnp.where(mine, pltpu.roll(a, 4 * i, 1) if i else a, low)
            high = jnp.where(mine, pltpu.roll(b, 4 * i + 4, 1), high)
        ZS[k, source, 0] = low
        ZS[k, source, 1] = high

    def send_sides(k, source, slot, section):
        for kind, side, there, yy, zz in sides:
            @pl.when(there)
            def _():
                side_copy(kind, side, k, source, slot, (section, yy, zz)).start()

    def wait_sides(k, slot):
        for kind, side, there, yy, zz in sides:
            @pl.when(there)
            def _():
                side_copy(kind, 1 - side, k, slot, slot, (p, yy, zz)).wait_recv()

    @pl.when(first)
    def _():
        for k in range(ITERS):
            pack(k, 0)
        for k in range(ITERS):
            send_sides(k, 0, 0, p)

    @pl.when(not_last)
    def _():
        ga_copy().start()

    @pl.when(first)
    def _():
        for v in range(NVAR):
            for b in range(2):
                cols = slice(b * LANES, (b + 1) * LANES)
                BD[v, b] = (1.0 - vig[v]) * (initial[0, v, :, cols] - inflow[v, :, cols])

    @pl.when(jnp.logical_not(first))
    def _():
        ga_copy().wait_recv()
        for v in range(NVAR):
            for b in range(2):
                cols = slice(b * LANES, (b + 1) * LANES)
                BD[v, b] = (1.0 - vig[v]) * (initial[0, v, :, cols] - GA[v, :, cols])

    def corrector(c, k):
        wait_sides(k, c)
        halo_left, halo_right = ZR[k, c, 0], ZR[k, c, 1]
        q = [[X[k, c, v, b, TOP:TOP + ROWS, :] for b in range(2)] for v in range(NVAR)]
        for v in range(NVAR):
            f = vig[v]
            speed = sz[v]
            const = direction(speed)
            pos = jnp.full((ROWS, LANES), speed, jnp.float32) >= 0.0
            halo = []
            for g in range(4):
                i = 4 * v + g
                r = pltpu.roll(halo_right, 128 - 4 * i, 1) if i else halo_right
                halo.append(jnp.where(lane < 64, r, pltpu.roll(halo_left, 124 - 4 * i, 1)))
            u = jnp.concatenate(q[v] + [jnp.concatenate(halo, 0)], 1)
            w = u.shape[1]
            flux = face(pltpu.roll(u, 2, 1), pltpu.roll(u, 1, 1), u,
                        pltpu.roll(u, w - 1, 1), pltpu.roll(u, w - 2, 1), const)
            before, after = pltpu.roll(flux, 1, 1), pltpu.roll(flux, w - 1, 1)
            for b in range(2):
                cols = slice(b * LANES, (b + 1) * LANES)
                div = speed * (jnp.where(pos, flux[:, cols], after[:, cols])
                               - jnp.where(pos, before[:, cols], flux[:, cols]))
                row_speed = sy[v]
                row_const = direction(row_speed)
                row_pos = jnp.full((ROWS, LANES), row_speed, jnp.float32) >= 0.0
                s = [X[k, c, v, b, TOP - 3 + o:TOP - 3 + o + ROWS + 2, :] for o in range(5)]
                rf = face(*s, row_const)
                f0, f1, f2 = rf[0:ROWS], rf[1:ROWS + 1], rf[2:ROWS + 2]
                div = div + row_speed * (jnp.where(row_pos, f1, f2) - jnp.where(row_pos, f0, f1))
                mixed = coup[v, 0] * q[0][b]
                for o in range(1, NVAR):
                    mixed = mixed + coup[v, o] * q[o][b]
                target = T0[v, b] + STEP_RATIO * (mixed - div)
                guess = q[v][b]
                for _ in range(NEWTON):
                    sq = guess * guess
                    r = inverse(1.0 + sq)
                    t = sq * r
                    value = guess + f * (guess * t)
                    slope = 1.0 + f * (t * ((3.0 + sq) * r))
                    guess = guess - (value - target) * inverse(slope)
                X[k, c + 1, v, b, TOP:TOP + ROWS, :] = jnp.where(
                    solid[0, :, cols] != 0, 0.0, guess)

            @pl.when((c == CORRECTORS - 1) & not_last)
            def _():
                plane_copy(k, v).start()

        @pl.when((c < CORRECTORS - 1) | not_last)
        def _():
            pack(k, c + 1)

        @pl.when(c < CORRECTORS - 1)
        def _():
            send_sides(k, c + 1, c + 1, p)

        @pl.when((c == CORRECTORS - 1) & not_last)
        def _():
            send_sides(k, c + 1, 0, p + 1)

        return k

    def iterate(k, carry):
        @pl.when(jnp.logical_not(first))
        def _():
            for v in range(NVAR):
                plane_copy(k, v).wait_recv()

        for v in range(NVAR):
            for b in range(2):
                up = X[k, 0, v, b, TOP:TOP + ROWS, :]
                sq = up * up
                T0[v, b] = up + vig[v] * (up * (sq * inverse(1.0 + sq))) - BD[v, b]
        lax.fori_loop(0, CORRECTORS, corrector, k)
        for v in range(NVAR):
            for b in range(2):
                BD[v, b] = (1.0 - vig[v]) * (X[k, 3, v, b, TOP:TOP + ROWS, :]
                                             - X[k, 0, v, b, TOP:TOP + ROWS, :])
        return carry

    lax.fori_loop(0, ITERS, iterate, 0)
    for v in range(NVAR):
        for b in range(2):
            out[0, v, :, b * LANES:(b + 1) * LANES] = X[ITERS - 1, 3, v, b, TOP:TOP + ROWS, :]

    @pl.when(not_last)
    def _():
        ga_copy().wait_send()

    def drain(k, carry):
        @pl.when(not_last)
        def _():
            for v in range(NVAR):
                plane_copy(k, v).wait_send()
        for kind, side, there, yy, zz in sides:
            @pl.when(there)
            def _():
                for source in (1, 2):
                    side_copy(kind, side, k, source, source, (p, yy, zz)).wait_send()

            @pl.when(there & first)
            def _():
                side_copy(kind, side, k, 0, 0, (p, yy, zz)).wait_send()

            @pl.when(there & not_last)
            def _():
                side_copy(kind, side, k, 3, 0, (p + 1, yy, zz)).wait_send()
        return carry

    lax.fori_loop(0, ITERS, drain, 0)


def per_device(inflow, initial, solid, speed_y, speed_z, vigneron, coupling):
    vmem = pl.BlockSpec(memory_space=pltpu.VMEM)
    smem = pl.BlockSpec(memory_space=pltpu.SMEM)
    plane = (NVAR, 2, ROWS, LANES)
    dma = pltpu.SemaphoreType.DMA
    return pl.pallas_call(
        kernel,
        out_shape=jax.ShapeDtypeStruct(initial.shape, jnp.float32),
        in_specs=[vmem] * 3 + [smem] * 4,
        out_specs=vmem,
        scratch_shapes=[
            pltpu.VMEM((ITERS, CORRECTORS + 1, NVAR, 2, 48, LANES), jnp.float32),
            pltpu.VMEM((NVAR, ROWS, 2 * LANES), jnp.float32),
            pltpu.VMEM(plane, jnp.float32),
            pltpu.VMEM(plane, jnp.float32),
            pltpu.VMEM((ITERS, CORRECTORS + 1, 2, 8, LANES), jnp.float32),
            pltpu.VMEM((ITERS, CORRECTORS, 2, 8, LANES), jnp.float32),
            dma((ITERS, CORRECTORS + 1, 2)),
            dma((ITERS, CORRECTORS, 2)),
            dma((ITERS, CORRECTORS + 1, 2)),
            dma((ITERS, CORRECTORS, 2)),
            dma((ITERS, NVAR)),
            dma((ITERS, NVAR)),
            dma,
            dma,
        ],
        compiler_params=pltpu.CompilerParams(collective_id=0, has_side_effects=True),
    )(inflow, initial, solid, speed_y, speed_z, vigneron, coupling)


def solution(mesh):
    return jax.shard_map(
        per_device,
        mesh=mesh,
        in_specs=(
            P(None, "gy", "gz"),
            P("sec", None, "gy", "gz"),
            P("sec", "gy", "gz"),
            P(),
            P(),
            P(),
            P(),
        ),
        out_specs=P("sec", None, "gy", "gz"),
        check_vma=False,
    )
```

```python
import jax
import jax.numpy as jnp
from jax import lax
from jax.experimental import pallas as pl
from jax.experimental.pallas import tpu as pltpu
from jax.sharding import PartitionSpec as P

ITERS = 4
CORRECTORS = 3
NEWTON = 2
NVAR = 5
STEP_RATIO = 0.25
WENO_EPS = 1e-06
ROWS = 32
LANES = 128
TOP = 8
MESH = pl.DeviceIdType.MESH


def inverse(x):
    r = pl.reciprocal(x, approx=True)
    return r * (2.0 - x * r)


def direction(speed):
    pos = speed >= 0.0

    def pick(a, b):
        return jnp.where(pos, jnp.float32(a), jnp.float32(b))

    return dict(
        s2=speed * speed,
        left=pick(1 / 6, 0.5),
        right=pick(0.5, 1 / 6),
        l1=pick(5 / 6, -4 / 6),
        l2=pick(-2 / 6, 1 / 6),
        m1=pick(1 / 6, -2 / 6),
        m2=pick(2 / 6, -1 / 6),
        r1=pick(4 / 6, -5 / 6),
        r2=pick(-1 / 6, 2 / 6),
    )


def face(a, b, c, d, e, k):
    ba, cb, dc, ed = b - a, c - b, d - c, e - d
    s2 = k["s2"]

    def weight(second, first):
        smooth = (13.0 / 3.0) * (second * second) + first * first
        r = inverse(4.0 * WENO_EPS + s2 * smooth)
        return r * r

    left2, mid2, right2 = cb - ba, dc - cb, ed - dc
    gl = k["left"] * weight(left2, left2 + 2.0 * cb)
    gm = weight(mid2, dc + cb)
    gr = k["right"] * weight(right2, right2 - 2.0 * dc)
    ql = k["l1"] * cb + k["l2"] * ba
    qm = k["m1"] * cb + k["m2"] * dc
    qr = k["r1"] * dc + k["r2"] * ed
    return c + (gl * ql + gm * qm + gr * qr) * inverse(gl + gm + gr)


def kernel(inflow, initial, solid, sy, sz, vig, coup, out,
           X, GA, BD, T0, T1, FS, YS, YR, ZS, ZR, ys_send, ys_recv, zs_send, zs_recv,
           pl_send, pl_recv, ga_send, ga_recv):
    p, y, z = lax.axis_index("sec"), lax.axis_index("gy"), lax.axis_index("gz")
    np_, ny, nz = lax.axis_size("sec"), lax.axis_size("gy"), lax.axis_size("gz")
    first, not_last = p == 0, p < np_ - 1
    sides = (
        ("y", 0, y > 0, y - 1, z), ("y", 1, y < ny - 1, y + 1, z),
        ("z", 0, z > 0, y, z - 1), ("z", 1, z < nz - 1, y, z + 1),
    )
    lane = lax.broadcasted_iota(jnp.int32, (8, LANES), 1)

    barrier = pltpu.get_barrier_semaphore()
    count = jnp.int32(0)
    for _, _, there, yy, zz in sides:
        count = count + there.astype(jnp.int32)

        @pl.when(there)
        def _():
            pl.semaphore_signal(barrier, inc=1, device_id=(p, yy, zz), device_id_type=MESH)

        @pl.when(there & (p > 0))
        def _():
            pl.semaphore_signal(barrier, inc=1, device_id=(p - 1, yy, zz), device_id_type=MESH)

    @pl.when(p > 0)
    def _():
        pl.semaphore_signal(barrier, inc=1, device_id=(p - 1, y, z), device_id_type=MESH)

    zero = jnp.zeros((8, LANES), jnp.float32)

    def clear(k, carry):
        for c in range(CORRECTORS):
            for v in range(NVAR):
                for b in range(2):
                    X[k, c, v, b, 0:TOP, :] = zero
                    X[k, c, v, b, TOP + ROWS:TOP + ROWS + 8, :] = zero
        return carry

    lax.fori_loop(0, ITERS, clear, 0)
    for kind, side, there, _, _ in sides:
        if kind == "z":
            @pl.when(jnp.logical_not(there))
            def _():
                for k in range(ITERS):
                    for c in range(CORRECTORS):
                        ZR[k, c, side] = zero

    @pl.when(first)
    def _():
        for v in range(NVAR):
            for b in range(2):
                q = inflow[v, :, b * LANES:(b + 1) * LANES]
                for k in range(ITERS):
                    X[k, 0, v, b, TOP:TOP + ROWS, :] = q

    pl.semaphore_wait(barrier, count + not_last.astype(jnp.int32) * (1 + count))

    def ga_copy():
        return pltpu.make_async_remote_copy(
            src_ref=initial.at[0], dst_ref=GA, send_sem=ga_send, recv_sem=ga_recv,
            device_id=(p + 1, y, z), device_id_type=MESH)

    def plane_copy(k, v):
        return pltpu.make_async_remote_copy(
            src_ref=X.at[k, 3, v, :, TOP:TOP + ROWS, :],
            dst_ref=X.at[k, 0, v, :, TOP:TOP + ROWS, :],
            send_sem=pl_send.at[k, v], recv_sem=pl_recv.at[k, v],
            device_id=(p + 1, y, z), device_id_type=MESH)

    def side_copy(kind, side, k, source, slot, target):
        other = 1 - side
        if kind == "y":
            return pltpu.make_async_remote_copy(
                src_ref=YS.at[k, source, side], dst_ref=YR.at[k, slot, other],
                send_sem=ys_send.at[k, source, side], recv_sem=ys_recv.at[k, slot, other],
                device_id=target, device_id_type=MESH)
        return pltpu.make_async_remote_copy(
            src_ref=ZS.at[k, source, side], dst_ref=ZR.at[k, slot, other],
            send_sem=zs_send.at[k, source, side], recv_sem=zs_recv.at[k, slot, other],
            device_id=target, device_id_type=MESH)

    def pack(k, source):
        low = jnp.zeros((8, LANES), jnp.float32)
        high = jnp.zeros((8, LANES), jnp.float32)
        for i in range(NVAR * 4):
            v, g = divmod(i, 4)
            rows = slice(TOP + 8 * g, TOP + 8 * g + 8)
            mine = (lane >= 4 * i) & (lane < 4 * i + 4)
            a = X[k, source, v, 0, rows, :]
            b = X[k, source, v, 1, rows, :]
            low = jnp.where(mine, pltpu.roll(a, 4 * i, 1) if i else a, low)
            high = jnp.where(mine, pltpu.roll(b, 4 * i + 4, 1), high)
        ZS[k, source, 0] = low
        ZS[k, source, 1] = high

    def send_sides(k, source, slot, section):
        for kind, side, there, yy, zz in sides:
            @pl.when(there)
            def _():
                side_copy(kind, side, k, source, slot, (section, yy, zz)).start()

    def wait_sides(which, k, slot):
        for kind, side, there, yy, zz in sides:
            if kind != which:
                continue

            @pl.when(there)
            def _():
                side_copy(kind, 1 - side, k, slot, slot, (p, yy, zz)).wait_recv()

    @pl.when(first)
    def _():
        for k in range(ITERS):
            for v in range(NVAR):
                for b in range(2):
                    rows = pl.ds(3 * (2 * v + b), 3)
                    cols = slice(b * LANES, (b + 1) * LANES)
                    YS[k, 0, 0, rows, :] = inflow[v, 0:3, cols]
                    YS[k, 0, 1, rows, :] = inflow[v, ROWS - 3:ROWS, cols]
            pack(k, 0)
        for k in range(ITERS):
            send_sides(k, 0, 0, p)

    @pl.when(not_last)
    def _():
        ga_copy().start()

    @pl.when(first)
    def _():
        for v in range(NVAR):
            for b in range(2):
                cols = slice(b * LANES, (b + 1) * LANES)
                BD[v, b] = (1.0 - vig[v]) * (initial[0, v, :, cols] - inflow[v, :, cols])

    @pl.when(jnp.logical_not(first))
    def _():
        ga_copy().wait_recv()
        for v in range(NVAR):
            for b in range(2):
                cols = slice(b * LANES, (b + 1) * LANES)
                BD[v, b] = (1.0 - vig[v]) * (initial[0, v, :, cols] - GA[v, :, cols])

    def corrector(c, k):
        def rows_of(v, b, at, count=8):
            return X[k, c, v, b, TOP + at:TOP + at + count, :]

        def row_face(v, b, at, const):
            return face(*[rows_of(v, b, at + o) for o in range(-2, 3)], const)

        y_const = [direction(sy[v]) for v in range(NVAR)]
        z_const = [direction(sz[v]) for v in range(NVAR)]
        y_pos = [jnp.full((8, LANES), sy[v], jnp.float32) >= 0.0 for v in range(NVAR)]

        for v in range(NVAR):
            for g in range(4):
                for b in range(2):
                    mixed = coup[v, 0] * rows_of(0, b, 8 * g)
                    for o in range(1, NVAR):
                        mixed = mixed + coup[v, o] * rows_of(o, b, 8 * g)
                    rows = slice(8 * g, 8 * g + 8)
                    T1[v, b, rows, :] = T0[v, b, rows, :] + STEP_RATIO * mixed
            for b in range(2):
                for g in range(4):
                    FS[v, b, TOP + 8 * g:TOP + 8 * g + 8, :] = row_face(v, b, 8 * g, y_const[v])

        wait_sides("y", k, c)
        for kind, side, there, _, _ in sides:
            if kind == "y":
                @pl.when(there)
                def _():
                    at = TOP - 3 if side == 0 else TOP + ROWS
                    for i in range(2 * NVAR):
                        X[k, c, i // 2, i % 2, at:at + 3, :] = YR[k, c, side, 3 * i:3 * i + 3, :]
        for v in range(NVAR):
            for b in range(2):
                for at in (-1, ROWS - 7):
                    FS[v, b, TOP + at:TOP + at + 8, :] = row_face(v, b, at, y_const[v])

        wait_sides("z", k, c)
        halo_left, halo_right = ZR[k, c, 0], ZR[k, c, 1]
        for v in range(NVAR):
            f = vig[v]
            pos = jnp.full((8, 2 * LANES), sz[v], jnp.float32) >= 0.0
            for g in range(4):
                i = 4 * v + g
                right = pltpu.roll(halo_right, LANES - 4 * i, 1) if i else halo_right
                halo = jnp.where(lane < 64, right, pltpu.roll(halo_left, 124 - 4 * i, 1))
                u = jnp.concatenate([rows_of(v, 0, 8 * g), rows_of(v, 1, 8 * g), halo], 1)
                w = u.shape[1]
                flux = face(pltpu.roll(u, 2, 1), pltpu.roll(u, 1, 1), u,
                            pltpu.roll(u, w - 1, 1), pltpu.roll(u, w - 2, 1), z_const[v])
                before, after = pltpu.roll(flux, 1, 1), pltpu.roll(flux, w - 1, 1)
                inner = slice(0, 2 * LANES)
                div = (STEP_RATIO * sz[v]) * jnp.where(
                    pos, (flux - before)[:, inner], (after - flux)[:, inner])
                for b in range(2):
                    rows = slice(8 * g, 8 * g + 8)
                    target = T1[v, b, rows, :] - div[:, b * LANES:(b + 1) * LANES]
                    f0, f1, f2 = [FS[v, b, TOP + 8 * g + o:TOP + 8 * g + o + 8, :] for o in (-1, 0, 1)]
                    target = target - (STEP_RATIO * sy[v]) * jnp.where(y_pos[v], f1 - f0, f2 - f1)
                    guess = rows_of(v, b, 8 * g)
                    for _ in range(NEWTON):
                        sq = guess * guess
                        r = inverse(1.0 + sq)
                        t = sq * r
                        value = guess + f * (guess * t)
                        slope = 1.0 + f * (t * ((3.0 + sq) * r))
                        guess = guess - (value - target) * inverse(slope)
                    guess = jnp.where(
                        solid[0, rows, b * LANES:(b + 1) * LANES] != 0, 0.0, guess)
                    X[k, c + 1, v, b, TOP + 8 * g:TOP + 8 * g + 8, :] = guess
                    at = pl.ds(3 * (2 * v + b), 3)
                    if g == 0:
                        YS[k, c + 1, 0, at, :] = guess[0:3]
                    if g == 3:
                        YS[k, c + 1, 1, at, :] = guess[5:8]

            @pl.when((c == CORRECTORS - 1) & not_last)
            def _():
                plane_copy(k, v).start()

        @pl.when((c < CORRECTORS - 1) | not_last)
        def _():
            pack(k, c + 1)

        @pl.when(c < CORRECTORS - 1)
        def _():
            send_sides(k, c + 1, c + 1, p)

        @pl.when((c == CORRECTORS - 1) & not_last)
        def _():
            send_sides(k, c + 1, 0, p + 1)

        return k

    def iterate(k, carry):
        @pl.when(jnp.logical_not(first))
        def _():
            for v in range(NVAR):
                plane_copy(k, v).wait_recv()

        for v in range(NVAR):
            for b in range(2):
                up = X[k, 0, v, b, TOP:TOP + ROWS, :]
                sq = up * up
                T0[v, b] = up + vig[v] * (up * (sq * inverse(1.0 + sq))) - BD[v, b]
        lax.fori_loop(0, CORRECTORS, corrector, k)
        for v in range(NVAR):
            for b in range(2):
                BD[v, b] = (1.0 - vig[v]) * (X[k, 3, v, b, TOP:TOP + ROWS, :]
                                             - X[k, 0, v, b, TOP:TOP + ROWS, :])
        return carry

    lax.fori_loop(0, ITERS, iterate, 0)
    for v in range(NVAR):
        for b in range(2):
            out[0, v, :, b * LANES:(b + 1) * LANES] = X[ITERS - 1, 3, v, b, TOP:TOP + ROWS, :]

    @pl.when(not_last)
    def _():
        ga_copy().wait_send()

    def drain(k, carry):
        @pl.when(not_last)
        def _():
            for v in range(NVAR):
                plane_copy(k, v).wait_send()
        for kind, side, there, yy, zz in sides:
            @pl.when(there)
            def _():
                for source in (1, 2):
                    side_copy(kind, side, k, source, source, (p, yy, zz)).wait_send()

            @pl.when(there & first)
            def _():
                side_copy(kind, side, k, 0, 0, (p, yy, zz)).wait_send()

            @pl.when(there & not_last)
            def _():
                side_copy(kind, side, k, 3, 0, (p + 1, yy, zz)).wait_send()
        return carry

    lax.fori_loop(0, ITERS, drain, 0)


def per_device(inflow, initial, solid, speed_y, speed_z, vigneron, coupling):
    vmem = pl.BlockSpec(memory_space=pltpu.VMEM)
    smem = pl.BlockSpec(memory_space=pltpu.SMEM)
    plane = (NVAR, 2, ROWS, LANES)
    dma = pltpu.SemaphoreType.DMA
    return pl.pallas_call(
        kernel,
        out_shape=jax.ShapeDtypeStruct(initial.shape, jnp.float32),
        in_specs=[vmem] * 3 + [smem] * 4,
        out_specs=vmem,
        scratch_shapes=[
            pltpu.VMEM((ITERS, CORRECTORS + 1, NVAR, 2, 48, LANES), jnp.float32),
            pltpu.VMEM((NVAR, ROWS, 2 * LANES), jnp.float32),
            pltpu.VMEM(plane, jnp.float32),
            pltpu.VMEM(plane, jnp.float32),
            pltpu.VMEM(plane, jnp.float32),
            pltpu.VMEM((NVAR, 2, 48, LANES), jnp.float32),
            pltpu.VMEM((ITERS, CORRECTORS + 1, 2, 32, LANES), jnp.float32),
            pltpu.VMEM((ITERS, CORRECTORS, 2, 32, LANES), jnp.float32),
            pltpu.VMEM((ITERS, CORRECTORS + 1, 2, 8, LANES), jnp.float32),
            pltpu.VMEM((ITERS, CORRECTORS, 2, 8, LANES), jnp.float32),
            dma((ITERS, CORRECTORS + 1, 2)),
            dma((ITERS, CORRECTORS, 2)),
            dma((ITERS, CORRECTORS + 1, 2)),
            dma((ITERS, CORRECTORS, 2)),
            dma((ITERS, NVAR)),
            dma((ITERS, NVAR)),
            dma,
            dma,
        ],
        compiler_params=pltpu.CompilerParams(collective_id=0, has_side_effects=True),
    )(inflow, initial, solid, speed_y, speed_z, vigneron, coupling)


def solution(mesh):
    return jax.shard_map(
        per_device,
        mesh=mesh,
        in_specs=(
            P(None, "gy", "gz"),
            P("sec", None, "gy", "gz"),
            P("sec", "gy", "gz"),
            P(),
            P(),
            P(),
            P(),
        ),
        out_specs=P("sec", None, "gy", "gz"),
        check_vma=False,
    )
```

```python
import jax
import jax.numpy as jnp
from jax import lax
from jax.experimental import pallas as pl
from jax.experimental.pallas import tpu as pltpu
from jax.sharding import PartitionSpec as P

ITERS = 4
CORRECTORS = 3
NEWTON = 2
NVAR = 5
STEP_RATIO = 0.25
WENO_EPS = 1e-06
ROWS = 32
LANES = 128
TOP = 8
MESH = pl.DeviceIdType.MESH


def inverse(x):
    r = pl.reciprocal(x, approx=True)
    return r * (2.0 - x * r)


def direction(speed):
    pos = speed >= 0.0

    def pick(a, b):
        return jnp.where(pos, jnp.float32(a), jnp.float32(b))

    return dict(
        s2=speed * speed,
        left=pick(1 / 6, 0.5),
        right=pick(0.5, 1 / 6),
        l1=pick(5 / 6, -4 / 6),
        l2=pick(-2 / 6, 1 / 6),
        m1=pick(1 / 6, -2 / 6),
        m2=pick(2 / 6, -1 / 6),
        r1=pick(4 / 6, -5 / 6),
        r2=pick(-1 / 6, 2 / 6),
    )


def face(a, b, c, d, e, k):
    ba, cb, dc, ed = b - a, c - b, d - c, e - d
    s2 = k["s2"]

    def weight(second, first):
        smooth = (13.0 / 3.0) * (second * second) + first * first
        r = inverse(4.0 * WENO_EPS + s2 * smooth)
        return r * r

    left2, mid2, right2 = cb - ba, dc - cb, ed - dc
    gl = k["left"] * weight(left2, left2 + 2.0 * cb)
    gm = weight(mid2, dc + cb)
    gr = k["right"] * weight(right2, right2 - 2.0 * dc)
    ql = k["l1"] * cb + k["l2"] * ba
    qm = k["m1"] * cb + k["m2"] * dc
    qr = k["r1"] * dc + k["r2"] * ed
    return c + (gl * ql + gm * qm + gr * qr) * inverse(gl + gm + gr)


def kernel(inflow, initial, solid, sy, sz, vig, coup, out,
           X, GA, BD, T0, T1, FS, YS, YR, ZS, ZR, ys_send, ys_recv, zs_send, zs_recv,
           pl_send, pl_recv, ga_send, ga_recv):
    p, y, z = lax.axis_index("sec"), lax.axis_index("gy"), lax.axis_index("gz")
    np_, ny, nz = lax.axis_size("sec"), lax.axis_size("gy"), lax.axis_size("gz")
    first, not_last = p == 0, p < np_ - 1
    sides = (
        ("y", 0, y > 0, y - 1, z), ("y", 1, y < ny - 1, y + 1, z),
        ("z", 0, z > 0, y, z - 1), ("z", 1, z < nz - 1, y, z + 1),
    )
    lane = lax.broadcasted_iota(jnp.int32, (8, LANES), 1)

    barrier = pltpu.get_barrier_semaphore()
    count = jnp.int32(0)
    for _, _, there, yy, zz in sides:
        count = count + there.astype(jnp.int32)

        @pl.when(there)
        def _():
            pl.semaphore_signal(barrier, inc=1, device_id=(p, yy, zz), device_id_type=MESH)

        @pl.when(there & (p > 0))
        def _():
            pl.semaphore_signal(barrier, inc=1, device_id=(p - 1, yy, zz), device_id_type=MESH)

    @pl.when(p > 0)
    def _():
        pl.semaphore_signal(barrier, inc=1, device_id=(p - 1, y, z), device_id_type=MESH)

    zero = jnp.zeros((8, LANES), jnp.float32)

    def clear(k, carry):
        for c in range(CORRECTORS):
            for v in range(NVAR):
                for b in range(2):
                    X[k, c, v, b, 0:TOP, :] = zero
                    X[k, c, v, b, TOP + ROWS:TOP + ROWS + 8, :] = zero
        return carry

    lax.fori_loop(0, ITERS, clear, 0)
    for kind, side, there, _, _ in sides:
        if kind == "z":
            @pl.when(jnp.logical_not(there))
            def _():
                for k in range(ITERS):
                    for c in range(CORRECTORS):
                        ZR[k, c, side] = zero

    @pl.when(first)
    def _():
        for v in range(NVAR):
            for b in range(2):
                q = inflow[v, :, b * LANES:(b + 1) * LANES]
                for k in range(ITERS):
                    X[k, 0, v, b, TOP:TOP + ROWS, :] = q

    pl.semaphore_wait(barrier, count + not_last.astype(jnp.int32) * (1 + count))

    def ga_copy():
        return pltpu.make_async_remote_copy(
            src_ref=initial.at[0], dst_ref=GA, send_sem=ga_send, recv_sem=ga_recv,
            device_id=(p + 1, y, z), device_id_type=MESH)

    def plane_copy(k, v):
        return pltpu.make_async_remote_copy(
            src_ref=X.at[k, 3, v, :, TOP:TOP + ROWS, :],
            dst_ref=X.at[k, 0, v, :, TOP:TOP + ROWS, :],
            send_sem=pl_send.at[k, v], recv_sem=pl_recv.at[k, v],
            device_id=(p + 1, y, z), device_id_type=MESH)

    def side_copy(kind, side, k, source, slot, target):
        other = 1 - side
        if kind == "y":
            return pltpu.make_async_remote_copy(
                src_ref=YS.at[k, source, side], dst_ref=YR.at[k, slot, other],
                send_sem=ys_send.at[k, source, side], recv_sem=ys_recv.at[k, slot, other],
                device_id=target, device_id_type=MESH)
        return pltpu.make_async_remote_copy(
            src_ref=ZS.at[k, source, side], dst_ref=ZR.at[k, slot, other],
            send_sem=zs_send.at[k, source, side], recv_sem=zs_recv.at[k, slot, other],
            device_id=target, device_id_type=MESH)

    def pack(k, source):
        low = jnp.zeros((8, LANES), jnp.float32)
        high = jnp.zeros((8, LANES), jnp.float32)
        for i in range(NVAR * 4):
            v, g = divmod(i, 4)
            rows = slice(TOP + 8 * g, TOP + 8 * g + 8)
            mine = (lane >= 4 * i) & (lane < 4 * i + 4)
            a = X[k, source, v, 0, rows, :]
            b = X[k, source, v, 1, rows, :]
            low = jnp.where(mine, pltpu.roll(a, 4 * i, 1) if i else a, low)
            high = jnp.where(mine, pltpu.roll(b, 4 * i + 4, 1), high)
        ZS[k, source, 0] = low
        ZS[k, source, 1] = high

    def send_sides(k, source, slot, section):
        for kind, side, there, yy, zz in sides:
            @pl.when(there)
            def _():
                side_copy(kind, side, k, source, slot, (section, yy, zz)).start()

    def wait_sides(which, k, slot):
        for kind, side, there, yy, zz in sides:
            if kind != which:
                continue

            @pl.when(there)
            def _():
                side_copy(kind, 1 - side, k, slot, slot, (p, yy, zz)).wait_recv()

    @pl.when(first)
    def _():
        for k in range(ITERS):
            for v in range(NVAR):
                for b in range(2):
                    rows = pl.ds(3 * (2 * v + b), 3)
                    cols = slice(b * LANES, (b + 1) * LANES)
                    YS[k, 0, 0, rows, :] = inflow[v, 0:3, cols]
                    YS[k, 0, 1, rows, :] = inflow[v, ROWS - 3:ROWS, cols]
            pack(k, 0)
        for k in range(ITERS):
            send_sides(k, 0, 0, p)

    @pl.when(not_last)
    def _():
        ga_copy().start()

    @pl.when(first)
    def _():
        for v in range(NVAR):
            for b in range(2):
                cols = slice(b * LANES, (b + 1) * LANES)
                BD[v, b] = (1.0 - vig[v]) * (initial[0, v, :, cols] - inflow[v, :, cols])

    @pl.when(jnp.logical_not(first))
    def _():
        ga_copy().wait_recv()
        for v in range(NVAR):
            for b in range(2):
                cols = slice(b * LANES, (b + 1) * LANES)
                BD[v, b] = (1.0 - vig[v]) * (initial[0, v, :, cols] - GA[v, :, cols])

    def corrector(c, k):
        def rows_of(v, b, at, count=8):
            return X[k, c, v, b, TOP + at:TOP + at + count, :]

        def row_face(v, b, at, const):
            return face(*[rows_of(v, b, at + o) for o in range(-2, 3)], const)

        y_const = [direction(sy[v]) for v in range(NVAR)]
        z_const = [direction(sz[v]) for v in range(NVAR)]
        y_pos = [jnp.full((8, LANES), sy[v], jnp.float32) >= 0.0 for v in range(NVAR)]

        for v in range(NVAR):
            for g in range(4):
                for b in range(2):
                    mixed = coup[v, 0] * rows_of(0, b, 8 * g)
                    for o in range(1, NVAR):
                        mixed = mixed + coup[v, o] * rows_of(o, b, 8 * g)
                    rows = slice(8 * g, 8 * g + 8)
                    T1[v, b, rows, :] = T0[v, b, rows, :] + STEP_RATIO * mixed
            for b in range(2):
                for g in range(4):
                    FS[v, b, TOP + 8 * g:TOP + 8 * g + 8, :] = row_face(v, b, 8 * g, y_const[v])

        wait_sides("y", k, c)
        for kind, side, there, _, _ in sides:
            if kind == "y":
                @pl.when(there)
                def _():
                    at = TOP - 3 if side == 0 else TOP + ROWS
                    for i in range(2 * NVAR):
                        X[k, c, i // 2, i % 2, at:at + 3, :] = YR[k, c, side, 3 * i:3 * i + 3, :]
        for v in range(NVAR):
            for b in range(2):
                for at in (-1, ROWS - 7):
                    FS[v, b, TOP + at:TOP + at + 8, :] = row_face(v, b, at, y_const[v])

        wait_sides("z", k, c)
        halo_left, halo_right = ZR[k, c, 0], ZR[k, c, 1]
        packed = [zero, zero]
        for v in range(NVAR):
            f = vig[v]
            pos = jnp.full((8, 2 * LANES), sz[v], jnp.float32) >= 0.0
            for g in range(4):
                i = 4 * v + g
                right = pltpu.roll(halo_right, LANES - 4 * i, 1) if i else halo_right
                halo = jnp.where(lane < 64, right, pltpu.roll(halo_left, 124 - 4 * i, 1))
                u = jnp.concatenate([rows_of(v, 0, 8 * g), rows_of(v, 1, 8 * g), halo], 1)
                w = u.shape[1]
                flux = face(pltpu.roll(u, 2, 1), pltpu.roll(u, 1, 1), u,
                            pltpu.roll(u, w - 1, 1), pltpu.roll(u, w - 2, 1), z_const[v])
                before, after = pltpu.roll(flux, 1, 1), pltpu.roll(flux, w - 1, 1)
                inner = slice(0, 2 * LANES)
                div = (STEP_RATIO * sz[v]) * jnp.where(
                    pos, (flux - before)[:, inner], (after - flux)[:, inner])
                for b in range(2):
                    rows = slice(8 * g, 8 * g + 8)
                    target = T1[v, b, rows, :] - div[:, b * LANES:(b + 1) * LANES]
                    f0, f1, f2 = [FS[v, b, TOP + 8 * g + o:TOP + 8 * g + o + 8, :] for o in (-1, 0, 1)]
                    target = target - (STEP_RATIO * sy[v]) * jnp.where(y_pos[v], f1 - f0, f2 - f1)
                    guess = rows_of(v, b, 8 * g)
                    for _ in range(NEWTON):
                        sq = guess * guess
                        r = inverse(1.0 + sq)
                        t = sq * r
                        value = guess + f * (guess * t)
                        slope = 1.0 + f * (t * ((3.0 + sq) * r))
                        guess = guess - (value - target) * inverse(slope)
                    guess = jnp.where(
                        solid[0, rows, b * LANES:(b + 1) * LANES] != 0, 0.0, guess)
                    X[k, c + 1, v, b, TOP + 8 * g:TOP + 8 * g + 8, :] = guess
                    mine = (lane >= 4 * i) & (lane < 4 * i + 4)
                    by = 4 * i + 4 * b
                    packed[b] = jnp.where(mine, pltpu.roll(guess, by, 1) if by else guess, packed[b])
                    at = pl.ds(3 * (2 * v + b), 3)
                    if g == 0:
                        YS[k, c + 1, 0, at, :] = guess[0:3]
                    if g == 3:
                        YS[k, c + 1, 1, at, :] = guess[5:8]

            @pl.when((c == CORRECTORS - 1) & not_last)
            def _():
                plane_copy(k, v).start()

        for b in range(2):
            ZS[k, c + 1, b] = packed[b]

        @pl.when(c < CORRECTORS - 1)
        def _():
            send_sides(k, c + 1, c + 1, p)

        @pl.when((c == CORRECTORS - 1) & not_last)
        def _():
            send_sides(k, c + 1, 0, p + 1)

        return k

    def iterate(k, carry):
        @pl.when(jnp.logical_not(first))
        def _():
            for v in range(NVAR):
                plane_copy(k, v).wait_recv()

        for v in range(NVAR):
            for b in range(2):
                up = X[k, 0, v, b, TOP:TOP + ROWS, :]
                sq = up * up
                T0[v, b] = up + vig[v] * (up * (sq * inverse(1.0 + sq))) - BD[v, b]
        lax.fori_loop(0, CORRECTORS, corrector, k)
        for v in range(NVAR):
            for b in range(2):
                BD[v, b] = (1.0 - vig[v]) * (X[k, 3, v, b, TOP:TOP + ROWS, :]
                                             - X[k, 0, v, b, TOP:TOP + ROWS, :])
        return carry

    lax.fori_loop(0, ITERS, iterate, 0)
    for v in range(NVAR):
        for b in range(2):
            out[0, v, :, b * LANES:(b + 1) * LANES] = X[ITERS - 1, 3, v, b, TOP:TOP + ROWS, :]

    @pl.when(not_last)
    def _():
        ga_copy().wait_send()

    def drain(k, carry):
        @pl.when(not_last)
        def _():
            for v in range(NVAR):
                plane_copy(k, v).wait_send()
        for kind, side, there, yy, zz in sides:
            @pl.when(there)
            def _():
                for source in (1, 2):
                    side_copy(kind, side, k, source, source, (p, yy, zz)).wait_send()

            @pl.when(there & first)
            def _():
                side_copy(kind, side, k, 0, 0, (p, yy, zz)).wait_send()

            @pl.when(there & not_last)
            def _():
                side_copy(kind, side, k, 3, 0, (p + 1, yy, zz)).wait_send()
        return carry

    lax.fori_loop(0, ITERS, drain, 0)


def per_device(inflow, initial, solid, speed_y, speed_z, vigneron, coupling):
    vmem = pl.BlockSpec(memory_space=pltpu.VMEM)
    smem = pl.BlockSpec(memory_space=pltpu.SMEM)
    plane = (NVAR, 2, ROWS, LANES)
    dma = pltpu.SemaphoreType.DMA
    return pl.pallas_call(
        kernel,
        out_shape=jax.ShapeDtypeStruct(initial.shape, jnp.float32),
        in_specs=[vmem] * 3 + [smem] * 4,
        out_specs=vmem,
        scratch_shapes=[
            pltpu.VMEM((ITERS, CORRECTORS + 1, NVAR, 2, 48, LANES), jnp.float32),
            pltpu.VMEM((NVAR, ROWS, 2 * LANES), jnp.float32),
            pltpu.VMEM(plane, jnp.float32),
            pltpu.VMEM(plane, jnp.float32),
            pltpu.VMEM(plane, jnp.float32),
            pltpu.VMEM((NVAR, 2, 48, LANES), jnp.float32),
            pltpu.VMEM((ITERS, CORRECTORS + 1, 2, 32, LANES), jnp.float32),
            pltpu.VMEM((ITERS, CORRECTORS, 2, 32, LANES), jnp.float32),
            pltpu.VMEM((ITERS, CORRECTORS + 1, 2, 8, LANES), jnp.float32),
            pltpu.VMEM((ITERS, CORRECTORS, 2, 8, LANES), jnp.float32),
            dma((ITERS, CORRECTORS + 1, 2)),
            dma((ITERS, CORRECTORS, 2)),
            dma((ITERS, CORRECTORS + 1, 2)),
            dma((ITERS, CORRECTORS, 2)),
            dma((ITERS, NVAR)),
            dma((ITERS, NVAR)),
            dma,
            dma,
        ],
        compiler_params=pltpu.CompilerParams(collective_id=0, has_side_effects=True),
    )(inflow, initial, solid, speed_y, speed_z, vigneron, coupling)


def solution(mesh):
    return jax.shard_map(
        per_device,
        mesh=mesh,
        in_specs=(
            P(None, "gy", "gz"),
            P("sec", None, "gy", "gz"),
            P("sec", "gy", "gz"),
            P(),
            P(),
            P(),
            P(),
        ),
        out_specs=P("sec", None, "gy", "gz"),
        check_vma=False,
    )
```
